32 devices in a mesh: grp: 8 (over y, x, core), tp: 4 (over z).
Axes of the slice: x: 2, y: 2, z: 4, core: 2. Of those that a mesh axis runs over, the one named last changes fastest.
Arguments:
- query: bfloat16 [16, 5120], P('grp'), may hold values from -6 to 6
- key_cache: bfloat16 [16, 512, 1024], P('grp', 'tp'), may hold values from -6 to 6
- value_cache: bfloat16 [16, 512, 1024], P('grp', 'tp'), may hold values from -6 to 6
- lengths: int32 [16], P('grp'), may hold values from 128 to 512
- route: int32 [16], replicated, may hold values from 0 to 15, each once
- out_weight: bfloat16 [5120, 5120], P(None, 'tp'), may hold values from -1.5 to 1.5
Outputs:
- inbox: bfloat16 [16, 5120], P('grp', 'tp')
The draws below stay inside these ranges and needn't reach their ends.
Inputs may be any that keep to these rules, and one draw needn't show every extreme that they name: lengths are at least one block of 128 positions. `route`: every inbox row is named by exactly one trajectory.
All inputs are finite; a program needn't handle non-finite values.
Results may differ from the reference program's by a relative error of at most 0.0095.
Values may be sent and summed in bfloat16 or wider, within the bound.
No kernel may reach another device: no remote copies, remote signals or barrier semaphores. Data moves between devices by JAX's collectives and lax.ppermute only.
A program may use at most 64 MiB of HBM per device.

```python
import jax
import jax.numpy as jnp
from jax import lax

D = 5120
HEADS = 40
KV_HEADS = 8
HEAD_DIM = 128
CTX_DEV = 128
CTX = 512
TRAJS = 16
N_TP = 4


def draw_query(key, part):
    sample = jax.random.truncated_normal(jax.random.fold_in(key, 11), -6.0, 6.0, (TRAJS, D), jnp.float32)
    return sample.astype(jnp.bfloat16)


def draw_key_cache(key, part):
    sample = jax.random.truncated_normal(jax.random.fold_in(key, 12), -6.0, 6.0, (TRAJS, CTX, KV_HEADS * HEAD_DIM), jnp.float32)
    return sample.astype(jnp.bfloat16)


def place_ends(values, own_key, low, top_value):
    longest = values.shape.index(max(values.shape))
    spots = []
    for shift in (0, 1):
        where = [jax.random.randint(jax.random.fold_in(own_key, axis), (), 0, length) for axis, length in enumerate(values.shape)]
        where[longest] = (where[longest] + shift) % values.shape[longest]
        spots.append(tuple(where))
    return values.at[spots[0]].set(low).at[spots[1]].set(top_value)


def block_levels(key, extent, shards, smallest, top_value):
    loudness, own = 1.0, jax.random.fold_in(key, 6)
    for axis_at, blocks in shards:
        steps = jnp.exp(jax.random.uniform(jax.random.fold_in(own, axis_at), (blocks,), jnp.float32, smallest / len(shards), top_value / len(shards)))
        loudness = loudness * jnp.repeat(steps, extent[axis_at] // blocks).reshape([-1 if axis == axis_at else 1 for axis in range(len(extent))])
    return loudness


def noise(rng, shape, deviation, bound, cuts=(), held_as=jnp.bfloat16):
    entries = deviation * jax.random.normal(rng, shape, jnp.float32)
    if cuts:
        entries = entries * block_levels(rng, shape, cuts, -0.22, 0.18)
    return jnp.clip(entries, -bound, bound).astype(held_as)


def setup_inputs(seed: int = 0) -> dict:
    streams_of = jax.random.split(jax.random.key(seed), 7)
    query = draw_query(jax.random.fold_in(streams_of[6], 71), 0)
    key_cache = draw_key_cache(jax.random.fold_in(streams_of[6], 71), 0)
    value_cache = noise(streams_of[2], (TRAJS, CTX, KV_HEADS * HEAD_DIM), 1.0, 6.0, ((0, 8), (1, 4)))
    lengths = place_ends(jax.random.randint(streams_of[3], (TRAJS,), CTX_DEV, CTX + 1), jax.random.fold_in(streams_of[3], 1), CTX_DEV, CTX).astype(jnp.int32)
    route = jax.random.permutation(streams_of[4], TRAJS).astype(jnp.int32)
    out_weight = noise(streams_of[5], (D, D), 16 ** -0.5, 1.5, ((1, 4),))
    return {"query": query, "key_cache": key_cache, "value_cache": value_cache, "lengths": lengths, "route": route, "out_weight": out_weight}


def one_trajectory(args):
    query_row, keys, values, length = args
    group = HEADS // KV_HEADS
    q = query_row.astype(jnp.float32).reshape(KV_HEADS, group, HEAD_DIM)
    k = keys.astype(jnp.float32).reshape(N_TP, CTX_DEV, KV_HEADS, HEAD_DIM)
    v = values.astype(jnp.float32).reshape(N_TP, CTX_DEV, KV_HEADS, HEAD_DIM)
    scores = jnp.einsum('kgd,btkd->bkgt', q, k) / jnp.sqrt(jnp.float32(HEAD_DIM))
    places = jnp.arange(CTX, dtype=jnp.int32).reshape(N_TP, 1, 1, CTX_DEV)
    live = places < length
    scores = jnp.where(live, scores, jnp.float32(-1e+30))
    blockmax = lax.optimization_barrier(jnp.max(scores, axis=3))
    expo = jnp.where(live, jnp.exp(scores - blockmax[..., None]), jnp.float32(0.0))
    blocksum = lax.optimization_barrier(jnp.sum(expo, axis=3))
    weights = expo.astype(jnp.bfloat16).astype(jnp.float32)
    blockout = jnp.einsum('bkgt,btkd->bkgd', weights, v)
    peak = lax.optimization_barrier(jnp.max(blockmax, axis=0))
    factor = jnp.exp(blockmax - peak[None])
    total = lax.optimization_barrier(jnp.sum(factor * blocksum, axis=0))
    combined = lax.optimization_barrier(jnp.sum(factor[..., None] * blockout, axis=0))
    return (combined / total[..., None]).reshape(D).astype(jnp.bfloat16)

def reference(query, key_cache, value_cache, lengths, route, out_weight):
    attended = lax.map(one_trajectory, (query, key_cache, value_cache, lengths))
    projected = jnp.dot(attended, out_weight, preferred_element_type=jnp.float32).astype(jnp.bfloat16)
    inbox = jnp.zeros((TRAJS, D), jnp.bfloat16).at[route].set(projected)
    return inbox
```

```python
import functools

import jax
import jax.numpy as jnp
from jax import lax
from jax.experimental import pallas as pl
from jax.experimental.pallas import tpu as pltpu
from jax.sharding import PartitionSpec as P

HEADS = 40
KV_HEADS = 8
HEAD_DIM = 128
GROUP = HEADS // KV_HEADS
LANES = 128
DEAD = -1e30

HBM = pltpu.MemorySpace.HBM
VMEM = pltpu.MemorySpace.VMEM


def attend_kernel(q_hbm, k_hbm, v_hbm, lengths_hbm, out_ref, q_ref, k_ref, v_ref, lengths_ref, sems):
    pairs = [(lengths_hbm, lengths_ref), (q_hbm, q_ref), (k_hbm, k_ref), (v_hbm, v_ref)]
    copies = [pltpu.make_async_copy(a, b, sems.at[i]) for i, (a, b) in enumerate(pairs)]
    for copy in copies:
        copy.start()
    rows, length = k_ref.shape[:2]
    first = lax.axis_index("tp") * length
    used = GROUP * rows
    tall = -(-used // 16) * 16
    scale = 1.0 / (HEAD_DIM**0.5)
    owner = lax.rem(lax.broadcasted_iota(jnp.int32, (tall, length), 0), rows)
    place = lax.broadcasted_iota(jnp.int32, (tall, length), 1)
    lane = lax.broadcasted_iota(jnp.int32, (tall, LANES), 1)
    home = lax.broadcasted_iota(jnp.int32, (tall, LANES), 0) // rows * KV_HEADS
    tops = jnp.zeros((tall, LANES), jnp.float32)
    sums = jnp.zeros((tall, LANES), jnp.float32)
    pad = jnp.zeros((tall - used, HEAD_DIM), jnp.float32)
    for copy in copies[:3]:
        copy.wait()
    limit = jnp.zeros((tall, length), jnp.int32)
    for b in range(rows):
        limit = jnp.where(owner == b, lengths_ref[b] - first, limit)
    live = place < limit
    q = q_ref[...].astype(jnp.float32)
    weights = []
    for k in range(KV_HEADS):
        span = pl.ds(k * HEAD_DIM, HEAD_DIM)
        heads = [slice((k * GROUP + g) * HEAD_DIM, (k * GROUP + g + 1) * HEAD_DIM) for g in range(GROUP)]
        queries = jnp.concatenate([q[:, h] for h in heads] + [pad], axis=0).astype(jnp.bfloat16)
        both = lax.dot_general(
            queries,
            k_ref[:, :, span].reshape(rows * length, HEAD_DIM),
            (((1,), (1,)), ((), ())),
            preferred_element_type=jnp.float32,
        )
        scores = both[:, :length]
        for b in range(1, rows):
            scores = jnp.where(owner == b, both[:, b * length : (b + 1) * length], scores)
        scores = jnp.where(live, scores * scale, jnp.float32(DEAD))
        top = jnp.max(scores, axis=1, keepdims=True)
        expo = jnp.where(live, jnp.exp(scores - top), jnp.float32(0.0))
        here = lane == home + k
        tops = jnp.where(here, top, tops)
        sums = jnp.where(here, jnp.sum(expo, axis=1, keepdims=True), sums)
        weights.append(
            jnp.concatenate(
                [jnp.where(owner == b, expo, jnp.float32(0.0)) for b in range(rows)], axis=1
            ).astype(jnp.bfloat16)
        )
    width = HEADS * HEAD_DIM
    out_ref[:, width : width + LANES] = functools.reduce(
        jnp.add, [tops[g * rows : (g + 1) * rows] for g in range(GROUP)]
    )
    out_ref[:, width + LANES :] = functools.reduce(
        jnp.add, [sums[g * rows : (g + 1) * rows] for g in range(GROUP)]
    )
    copies[3].wait()
    for k in range(KV_HEADS):
        span = pl.ds(k * HEAD_DIM, HEAD_DIM)
        out = jnp.dot(
            weights[k],
            v_ref[:, :, span].reshape(rows * length, HEAD_DIM),
            preferred_element_type=jnp.float32,
        )
        for g in range(GROUP):
            head = k * GROUP + g
            out_ref[:, head * HEAD_DIM : (head + 1) * HEAD_DIM] = out[g * rows : (g + 1) * rows]


def project_kernel(sources, route_hbm, weight_ref, *refs):
    messages = refs[:sources]
    out_ref, attended, route_ref, sem = refs[sources:]
    slots, rows, cols = out_ref.shape
    depth = weight_ref.shape[0]
    fetch = pltpu.make_async_copy(route_hbm, route_ref, sem)
    fetch.start()
    tops = [m[:, depth : depth + LANES] for m in messages]
    sums = [m[:, depth + LANES :] for m in messages]
    peak = functools.reduce(jnp.maximum, tops)
    factors = [jnp.exp(top - peak) for top in tops]
    total = functools.reduce(jnp.add, [f * s for f, s in zip(factors, sums)])
    shares = [f / total for f in factors]
    attended[...] = jnp.zeros_like(attended)
    for head in range(HEADS):
        k, g = divmod(head, GROUP)
        lane = KV_HEADS * g + k
        span = slice(head * HEAD_DIM, (head + 1) * HEAD_DIM)
        attended[:rows, span] = functools.reduce(
            jnp.add, [m[:, span] * s[:, lane : lane + 1] for m, s in zip(messages, shares)]
        )
    acc = jnp.dot(
        attended[...].astype(jnp.bfloat16), weight_ref[...], preferred_element_type=jnp.float32
    )
    fetch.wait()
    mine = lax.axis_index("grp") * rows
    slot_row = lax.broadcasted_iota(jnp.int32, (rows, cols), 0)
    for s in range(slots):
        placed = jnp.zeros((rows, cols), jnp.float32)
        for b in range(rows):
            placed = jnp.where(slot_row == route_ref[mine + b] - s * rows, acc[b : b + 1], placed)
        out_ref[s] = placed.astype(jnp.bfloat16)


def body(tp, grp, query, key_cache, value_cache, lengths, route, out_weight):
    rows, depth = query.shape
    cols = out_weight.shape[1]
    here = pl.BlockSpec(memory_space=VMEM)
    there = pl.BlockSpec(memory_space=HBM)
    inputs = [pltpu.with_memory_space_constraint(x, HBM) for x in (query, key_cache, value_cache, lengths)]
    message = pl.pallas_call(
        attend_kernel,
        out_shape=jax.ShapeDtypeStruct((rows, depth + 2 * LANES), jnp.float32),
        in_specs=[there] * 4,
        out_specs=here,
        scratch_shapes=[
            pltpu.VMEM(query.shape, query.dtype),
            pltpu.VMEM(key_cache.shape, key_cache.dtype),
            pltpu.VMEM(value_cache.shape, value_cache.dtype),
            pltpu.SMEM(lengths.shape, lengths.dtype),
            pltpu.SemaphoreType.DMA((4,)),
        ],
        compiler_params=pltpu.CompilerParams(vmem_limit_bytes=8 << 20),
        cost_estimate=pl.CostEstimate(
            flops=20_000_000_000, transcendentals=0, bytes_accessed=40_000_000
        ),
        name="attend",
    )(*inputs)
    if tp & (tp - 1) == 0 and tp <= 4:
        messages = [message] + [
            lax.ppermute(message, "tp", [(i, i ^ s) for i in range(tp)]) for s in range(1, tp)
        ]
    else:
        gathered = lax.all_gather(message, "tp", axis=0)
        messages = [gathered[i] for i in range(tp)]
    outgoing = pl.pallas_call(
        functools.partial(project_kernel, tp),
        out_shape=jax.ShapeDtypeStruct((grp, rows, cols), jnp.bfloat16),
        in_specs=[there] + [here] * (tp + 1),
        out_specs=here,
        scratch_shapes=[
            pltpu.VMEM((16, depth), jnp.float32),
            pltpu.SMEM(route.shape, route.dtype),
            pltpu.SemaphoreType.DMA,
        ],
        compiler_params=pltpu.CompilerParams(vmem_limit_bytes=24 << 20),
        name="project",
    )(pltpu.with_memory_space_constraint(route, HBM), out_weight, *messages)
    incoming = lax.all_to_all(outgoing, "grp", 0, 0)
    return jnp.sum(incoming.astype(jnp.float32), axis=0).astype(jnp.bfloat16)


def solution(mesh):
    return jax.shard_map(
        functools.partial(body, mesh.shape["tp"], mesh.shape["grp"]),
        mesh=mesh,
        in_specs=(
            P("grp", None),
            P("grp", "tp", None),
            P("grp", "tp", None),
            P("grp"),
            P(),
            P(None, "tp"),
        ),
        out_specs=P("grp", "tp"),
        check_vma=False,
    )
```

```python
import functools

import jax
import jax.numpy as jnp
from jax import lax
from jax.experimental import pallas as pl
from jax.experimental.pallas import tpu as pltpu
from jax.sharding import PartitionSpec as P

HEADS = 40
KV_HEADS = 8
HEAD_DIM = 128
GROUP = HEADS // KV_HEADS
LANES = 128
DEAD = -1e30
EXTRA = 3 * LANES
OVER_TP = ((1, 0, 3, 2), (3, 2, 0, 1), (2, 3, 1, 0))

HBM = pltpu.MemorySpace.HBM
VMEM = pltpu.MemorySpace.VMEM


def attend_kernel(q_hbm, k_hbm, v_hbm, lengths_hbm, out_ref, q_ref, k_ref, v_ref, lengths_ref, sems):
    pairs = [(lengths_hbm, lengths_ref), (q_hbm, q_ref), (k_hbm, k_ref), (v_hbm, v_ref)]
    copies = [pltpu.make_async_copy(a, b, sems.at[i]) for i, (a, b) in enumerate(pairs)]
    for copy in copies:
        copy.start()
    rows, length = k_ref.shape[:2]
    first = lax.axis_index("tp") * length
    used = GROUP * rows
    tall = -(-used // 16) * 16
    scale = 1.0 / (HEAD_DIM**0.5)
    owner = lax.rem(lax.broadcasted_iota(jnp.int32, (tall, length), 0), rows)
    place = lax.broadcasted_iota(jnp.int32, (tall, length), 1)
    lane = lax.broadcasted_iota(jnp.int32, (tall, LANES), 1)
    home = lax.broadcasted_iota(jnp.int32, (tall, LANES), 0) // rows * KV_HEADS
    tops = jnp.zeros((tall, LANES), jnp.float32)
    sums = jnp.zeros((tall, LANES), jnp.float32)
    pad = jnp.zeros((tall - used, HEAD_DIM), jnp.float32)
    for copy in copies[:3]:
        copy.wait()
    limit = jnp.zeros((tall, length), jnp.int32)
    for b in range(rows):
        limit = jnp.where(owner == b, lengths_ref[b] - first, limit)
    live = place < limit
    q = q_ref[...].astype(jnp.float32)
    weights = []
    for k in range(KV_HEADS):
        span = pl.ds(k * HEAD_DIM, HEAD_DIM)
        heads = [slice((k * GROUP + g) * HEAD_DIM, (k * GROUP + g + 1) * HEAD_DIM) for g in range(GROUP)]
        queries = jnp.concatenate([q[:, h] for h in heads] + [pad], axis=0).astype(jnp.bfloat16)
        both = lax.dot_general(
            queries,
            k_ref[:, :, span].reshape(rows * length, HEAD_DIM),
            (((1,), (1,)), ((), ())),
            preferred_element_type=jnp.float32,
        )
        scores = both[:, :length]
        for b in range(1, rows):
            scores = jnp.where(owner == b, both[:, b * length : (b + 1) * length], scores)
        scores = jnp.where(live, scores * scale, jnp.float32(DEAD))
        top = jnp.max(scores, axis=1, keepdims=True).astype(jnp.bfloat16).astype(jnp.float32)
        expo = jnp.where(live, jnp.exp(scores - top), jnp.float32(0.0))
        here = lane == home + k
        tops = jnp.where(here, top, tops)
        sums = jnp.where(here, jnp.sum(expo, axis=1, keepdims=True), sums)
        weights.append(
            jnp.concatenate(
                [jnp.where(owner == b, expo, jnp.float32(0.0)) for b in range(rows)], axis=1
            ).astype(jnp.bfloat16)
        )
    width = HEADS * HEAD_DIM
    top = functools.reduce(jnp.add, [tops[g * rows : (g + 1) * rows] for g in range(GROUP)])
    total = functools.reduce(jnp.add, [sums[g * rows : (g + 1) * rows] for g in range(GROUP)])
    high = total.astype(jnp.bfloat16)
    low = (total - high.astype(jnp.float32)).astype(jnp.bfloat16)
    for i, part in enumerate((top.astype(jnp.bfloat16), high, low)):
        out_ref[:, width + i * LANES : width + (i + 1) * LANES] = part
    copies[3].wait()
    for k in range(KV_HEADS):
        span = pl.ds(k * HEAD_DIM, HEAD_DIM)
        out = jnp.dot(
            weights[k],
            v_ref[:, :, span].reshape(rows * length, HEAD_DIM),
            preferred_element_type=jnp.float32,
        )
        for g in range(GROUP):
            head = k * GROUP + g
            out_ref[:, head * HEAD_DIM : (head + 1) * HEAD_DIM] = (
                out[g * rows : (g + 1) * rows].astype(jnp.bfloat16)
            )


def project_kernel(sources, route_hbm, weight_ref, *refs):
    messages = refs[:sources]
    out_ref, attended, route_ref, sem = refs[sources:]
    slots, rows, cols = out_ref.shape
    depth = weight_ref.shape[0]
    fetch = pltpu.make_async_copy(route_hbm, route_ref, sem)
    fetch.start()
    tops, highs, lows = (
        [m[:, depth + i * LANES : depth + (i + 1) * LANES].astype(jnp.float32) for m in messages]
        for i in range(3)
    )
    sums = [high + low for high, low in zip(highs, lows)]
    peak = functools.reduce(jnp.maximum, tops)
    factors = [jnp.exp(top - peak) for top in tops]
    total = functools.reduce(jnp.add, [f * s for f, s in zip(factors, sums)])
    shares = [f / total for f in factors]
    attended[...] = jnp.zeros_like(attended)
    for head in range(HEADS):
        k, g = divmod(head, GROUP)
        lane = KV_HEADS * g + k
        span = slice(head * HEAD_DIM, (head + 1) * HEAD_DIM)
        attended[:rows, span] = functools.reduce(
            jnp.add, [
                m[:, span].astype(jnp.float32) * s[:, lane : lane + 1]
                for m, s in zip(messages, shares)
            ]
        )
    acc = jnp.dot(
        attended[...].astype(jnp.bfloat16), weight_ref[...], preferred_element_type=jnp.float32
    )
    fetch.wait()
    mine = lax.axis_index("grp") * rows
    slot_row = lax.broadcasted_iota(jnp.int32, (rows, cols), 0)
    for s in range(slots):
        placed = jnp.zeros((rows, cols), jnp.float32)
        for b in range(rows):
            placed = jnp.where(slot_row == route_ref[mine + b] - s * rows, acc[b : b + 1], placed)
        out_ref[s] = placed.astype(jnp.bfloat16)


def body(tp, grp, query, key_cache, value_cache, lengths, route, out_weight):
    rows, depth = query.shape
    cols = out_weight.shape[1]
    here = pl.BlockSpec(memory_space=VMEM)
    there = pl.BlockSpec(memory_space=HBM)
    inputs = [pltpu.with_memory_space_constraint(x, HBM) for x in (query, key_cache, value_cache, lengths)]
    message = pl.pallas_call(
        attend_kernel,
        out_shape=jax.ShapeDtypeStruct((rows, depth + EXTRA), jnp.bfloat16),
        in_specs=[there] * 4,
        out_specs=here,
        scratch_shapes=[
            pltpu.VMEM(query.shape, query.dtype),
            pltpu.VMEM(key_cache.shape, key_cache.dtype),
            pltpu.VMEM(value_cache.shape, value_cache.dtype),
            pltpu.SMEM(lengths.shape, lengths.dtype),
            pltpu.SemaphoreType.DMA((4,)),
        ],
        compiler_params=pltpu.CompilerParams(vmem_limit_bytes=8 << 20),
        cost_estimate=pl.CostEstimate(
            flops=20_000_000_000, transcendentals=0, bytes_accessed=40_000_000
        ),
        name="attend",
    )(*inputs)
    if tp == len(OVER_TP[0]):
        steps = [[(i, step[i]) for i in range(tp)] for step in OVER_TP]
        messages = [message] + [lax.ppermute(message, "tp", step) for step in steps]
    else:
        gathered = lax.all_gather(message, "tp", axis=0)
        messages = [gathered[i] for i in range(tp)]
    outgoing = pl.pallas_call(
        functools.partial(project_kernel, tp),
        out_shape=jax.ShapeDtypeStruct((grp, rows, cols), jnp.bfloat16),
        in_specs=[there] + [here] * (tp + 1),
        out_specs=here,
        scratch_shapes=[
            pltpu.VMEM((16, depth), jnp.float32),
            pltpu.SMEM(route.shape, route.dtype),
            pltpu.SemaphoreType.DMA,
        ],
        compiler_params=pltpu.CompilerParams(vmem_limit_bytes=24 << 20),
        name="project",
    )(pltpu.with_memory_space_constraint(route, HBM), out_weight, *messages)
    incoming = lax.all_to_all(outgoing, "grp", 0, 0)
    return jnp.sum(incoming.astype(jnp.float32), axis=0).astype(jnp.bfloat16)


def solution(mesh):
    return jax.shard_map(
        functools.partial(body, mesh.shape["tp"], mesh.shape["grp"]),
        mesh=mesh,
        in_specs=(
            P("grp", None),
            P("grp", "tp", None),
            P("grp", "tp", None),
            P("grp"),
            P(),
            P(None, "tp"),
        ),
        out_specs=P("grp", "tp"),
        check_vma=False,
    )
```

```python
import functools

import jax
import jax.numpy as jnp
from jax import lax
from jax.experimental import pallas as pl
from jax.experimental.pallas import tpu as pltpu
from jax.sharding import PartitionSpec as P

HEADS = 40
KV_HEADS = 8
HEAD_DIM = 128
GROUP = HEADS // KV_HEADS
LANES = 128
DEAD = -1e30
EXTRA = 3 * LANES
OVER_CHIPS = ((2, 3, 1, 0), (3, 2, 0, 1), (1, 0, 3, 2))
CORES = 2
OVER_TP = ((1, 0, 3, 2), (3, 2, 0, 1), (2, 3, 1, 0))

HBM = pltpu.MemorySpace.HBM
VMEM = pltpu.MemorySpace.VMEM


def attend_kernel(q_hbm, k_hbm, v_hbm, lengths_hbm, out_ref, q_ref, k_ref, v_ref, lengths_ref, sems):
    pairs = [(lengths_hbm, lengths_ref), (q_hbm, q_ref), (k_hbm, k_ref), (v_hbm, v_ref)]
    copies = [pltpu.make_async_copy(a, b, sems.at[i]) for i, (a, b) in enumerate(pairs)]
    for copy in copies:
        copy.start()
    rows, length = k_ref.shape[:2]
    first = lax.axis_index("tp") * length
    used = GROUP * rows
    tall = -(-used // 16) * 16
    scale = 1.0 / (HEAD_DIM**0.5)
    owner = lax.rem(lax.broadcasted_iota(jnp.int32, (tall, length), 0), rows)
    place = lax.broadcasted_iota(jnp.int32, (tall, length), 1)
    lane = lax.broadcasted_iota(jnp.int32, (tall, LANES), 1)
    home = lax.broadcasted_iota(jnp.int32, (tall, LANES), 0) // rows * KV_HEADS
    tops = jnp.zeros((tall, LANES), jnp.float32)
    sums = jnp.zeros((tall, LANES), jnp.float32)
    pad = jnp.zeros((tall - used, HEAD_DIM), jnp.float32)
    for copy in copies[:3]:
        copy.wait()
    limit = jnp.zeros((tall, length), jnp.int32)
    for b in range(rows):
        limit = jnp.where(owner == b, lengths_ref[b] - first, limit)
    live = place < limit
    q = q_ref[...].astype(jnp.float32)
    weights = []
    for k in range(KV_HEADS):
        span = pl.ds(k * HEAD_DIM, HEAD_DIM)
        heads = [slice((k * GROUP + g) * HEAD_DIM, (k * GROUP + g + 1) * HEAD_DIM) for g in range(GROUP)]
        queries = jnp.concatenate([q[:, h] for h in heads] + [pad], axis=0).astype(jnp.bfloat16)
        both = lax.dot_general(
            queries,
            k_ref[:, :, span].reshape(rows * length, HEAD_DIM),
            (((1,), (1,)), ((), ())),
            preferred_element_type=jnp.float32,
        )
        scores = both[:, :length]
        for b in range(1, rows):
            scores = jnp.where(owner == b, both[:, b * length : (b + 1) * length], scores)
        scores = jnp.where(live, scores * scale, jnp.float32(DEAD))
        top = jnp.max(scores, axis=1, keepdims=True).astype(jnp.bfloat16).astype(jnp.float32)
        expo = jnp.where(live, jnp.exp(scores - top), jnp.float32(0.0))
        here = lane == home + k
        tops = jnp.where(here, top, tops)
        sums = jnp.where(here, jnp.sum(expo, axis=1, keepdims=True), sums)
        weights.append(
            jnp.concatenate(
                [jnp.where(owner == b, expo, jnp.float32(0.0)) for b in range(rows)], axis=1
            ).astype(jnp.bfloat16)
        )
    width = HEADS * HEAD_DIM
    top = functools.reduce(jnp.add, [tops[g * rows : (g + 1) * rows] for g in range(GROUP)])
    total = functools.reduce(jnp.add, [sums[g * rows : (g + 1) * rows] for g in range(GROUP)])
    high = total.astype(jnp.bfloat16)
    low = (total - high.astype(jnp.float32)).astype(jnp.bfloat16)
    for i, part in enumerate((top.astype(jnp.bfloat16), high, low)):
        out_ref[:, width + i * LANES : width + (i + 1) * LANES] = part
    copies[3].wait()
    for k in range(KV_HEADS):
        span = pl.ds(k * HEAD_DIM, HEAD_DIM)
        out = jnp.dot(
            weights[k],
            v_ref[:, :, span].reshape(rows * length, HEAD_DIM),
            preferred_element_type=jnp.float32,
        )
        for g in range(GROUP):
            head = k * GROUP + g
            out_ref[:, head * HEAD_DIM : (head + 1) * HEAD_DIM] = (
                out[g * rows : (g + 1) * rows].astype(jnp.bfloat16)
            )


def project_kernel(sources, crossed, route_hbm, weight_ref, *refs):
    messages = refs[:sources]
    *outs, attended, route_ref, sem = refs[sources:]
    rows, cols = outs[0].shape[1:]
    depth = weight_ref.shape[0]
    fetch = pltpu.make_async_copy(route_hbm, route_ref, sem)
    fetch.start()
    tops, highs, lows = (
        [m[:, depth + i * LANES : depth + (i + 1) * LANES].astype(jnp.float32) for m in messages]
        for i in range(3)
    )
    sums = [high + low for high, low in zip(highs, lows)]
    peak = functools.reduce(jnp.maximum, tops)
    factors = [jnp.exp(top - peak) for top in tops]
    total = functools.reduce(jnp.add, [f * s for f, s in zip(factors, sums)])
    shares = [f / total for f in factors]
    attended[...] = jnp.zeros_like(attended)
    for head in range(HEADS):
        k, g = divmod(head, GROUP)
        lane = KV_HEADS * g + k
        span = slice(head * HEAD_DIM, (head + 1) * HEAD_DIM)
        attended[:rows, span] = functools.reduce(
            jnp.add, [
                m[:, span].astype(jnp.float32) * s[:, lane : lane + 1]
                for m, s in zip(messages, shares)
            ]
        )
    acc = jnp.dot(
        attended[...].astype(jnp.bfloat16), weight_ref[...], preferred_element_type=jnp.float32
    )
    fetch.wait()
    place = lax.axis_index("grp")
    mine = place + 1 - 2 * lax.rem(place, CORES) if crossed else place
    targets = [route_ref[mine * rows + b] for b in range(rows)]
    slot_row = lax.broadcasted_iota(jnp.int32, (rows, cols), 0)

    def placed(slot):
        out = jnp.zeros((rows, cols), jnp.float32)
        for b in range(rows):
            out = jnp.where(slot_row == targets[b] - slot * rows, acc[b : b + 1], out)
        return out.astype(jnp.bfloat16)

    if len(outs) == 1:
        for slot in range(outs[0].shape[0]):
            outs[0][slot] = placed(slot)
    else:
        chip, core = place // CORES, lax.rem(place, CORES)
        for step, out in zip((range(len(outs)), *OVER_CHIPS), outs):
            goal = functools.reduce(lambda a, i: jnp.where(chip == i, step[i], a), range(len(step)), 0)
            taker = core if out is outs[0] else 1 - core
            out[0] = placed(goal * CORES + taker)
            out[1] = placed(goal * CORES + 1 - taker)


def relay_kernel(*refs):
    refs[-1][...] = functools.reduce(jnp.add, [r[1].astype(jnp.float32) for r in refs[:-1]]).astype(
        jnp.bfloat16
    )


def collect_kernel(*refs):
    parts = [r[0].astype(jnp.float32) for r in refs[:-2]] + [refs[-2][...].astype(jnp.float32)]
    refs[-1][...] = functools.reduce(jnp.add, parts).astype(jnp.bfloat16)


def body(tp, grp, query, key_cache, value_cache, lengths, route, out_weight):
    rows, depth = query.shape
    cols = out_weight.shape[1]
    here = pl.BlockSpec(memory_space=VMEM)
    there = pl.BlockSpec(memory_space=HBM)
    inputs = [pltpu.with_memory_space_constraint(x, HBM) for x in (query, key_cache, value_cache, lengths)]
    message = pl.pallas_call(
        attend_kernel,
        out_shape=jax.ShapeDtypeStruct((rows, depth + EXTRA), jnp.bfloat16),
        in_specs=[there] * 4,
        out_specs=here,
        scratch_shapes=[
            pltpu.VMEM(query.shape, query.dtype),
            pltpu.VMEM(key_cache.shape, key_cache.dtype),
            pltpu.VMEM(value_cache.shape, value_cache.dtype),
            pltpu.SMEM(lengths.shape, lengths.dtype),
            pltpu.SemaphoreType.DMA((4,)),
        ],
        compiler_params=pltpu.CompilerParams(vmem_limit_bytes=8 << 20),
        cost_estimate=pl.CostEstimate(
            flops=20_000_000_000, transcendentals=0, bytes_accessed=40_000_000
        ),
        name="attend",
    )(*inputs)
    crossed = tp == len(OVER_TP[0]) and grp % CORES == 0
    if crossed:
        swap = [(g, g ^ 1) for g in range(grp)]
        messages = [lax.ppermute(message, "grp", swap)]
        for step in OVER_TP:
            pairs = [(g * tp + t, (g ^ 1) * tp + step[t]) for g in range(grp) for t in range(tp)]
            messages.append(lax.ppermute(message, ("grp", "tp"), pairs))
    else:
        gathered = lax.all_gather(message, "tp", axis=0)
        messages = [gathered[i] for i in range(tp)]
    chips = len(OVER_CHIPS[0])
    by_steps = grp == chips * CORES
    shape = jax.ShapeDtypeStruct((CORES if by_steps else grp, rows, cols), jnp.bfloat16)
    outgoing = pl.pallas_call(
        functools.partial(project_kernel, tp, crossed),
        out_shape=[shape] * (chips if by_steps else 1),
        in_specs=[there] + [here] * (tp + 1),
        out_specs=[here] * (chips if by_steps else 1),
        scratch_shapes=[
            pltpu.VMEM((16, depth), jnp.float32),
            pltpu.SMEM(route.shape, route.dtype),
            pltpu.SemaphoreType.DMA,
        ],
        compiler_params=pltpu.CompilerParams(vmem_limit_bytes=24 << 20),
        name="project",
    )(pltpu.with_memory_space_constraint(route, HBM), out_weight, *messages)
    if not by_steps:
        incoming = lax.all_to_all(outgoing[0], "grp", 0, 0)
        return jnp.sum(incoming.astype(jnp.float32), axis=0).astype(jnp.bfloat16)
    got = [outgoing[0]]
    for step, block in zip(OVER_CHIPS, outgoing[1:]):
        pairs = [(i * CORES + c, step[i] * CORES + 1 - c) for i in range(chips) for c in range(CORES)]
        got.append(lax.ppermute(block, "grp", pairs))
    row_block = jax.ShapeDtypeStruct((rows, cols), jnp.bfloat16)
    partners = pl.pallas_call(
        relay_kernel,
        out_shape=row_block,
        in_specs=[here] * chips,
        out_specs=here,
        compiler_params=pltpu.CompilerParams(vmem_limit_bytes=1 << 20),
        name="relay",
    )(*got)
    swap = [(i, i ^ 1) for i in range(grp)]
    return pl.pallas_call(
        collect_kernel,
        out_shape=row_block,
        in_specs=[here] * (chips + 1),
        out_specs=here,
        compiler_params=pltpu.CompilerParams(vmem_limit_bytes=1 << 20),
        name="collect",
    )(*got, lax.ppermute(partners, "grp", swap))


def solution(mesh):
    return jax.shard_map(
        functools.partial(body, mesh.shape["tp"], mesh.shape["grp"]),
        mesh=mesh,
        in_specs=(
            P("grp", None),
            P("grp", "tp", None),
            P("grp", "tp", None),
            P("grp"),
            P(),
            P(None, "tp"),
        ),
        out_specs=P("grp", "tp"),
        check_vma=False,
    )
```

```python
import functools

import jax
import jax.numpy as jnp
from jax import lax
from jax.experimental import pallas as pl
from jax.experimental.pallas import tpu as pltpu
from jax.sharding import PartitionSpec as P

HEADS = 40
KV_HEADS = 8
HEAD_DIM = 128
GROUP = HEADS // KV_HEADS
LANES = 128
PER_DOT = 2
DEAD = -1e30
EXTRA = 3 * LANES
OVER_CHIPS = (
    ((1, 2, 3, 0), (3, 0, 1, 2), (2, 3, 0, 1)),
    ((2, 3, 1, 0), (3, 2, 0, 1), (1, 0, 3, 2)),
)
CORES = 2
OVER_TP = ((1, 0, 3, 2), (3, 2, 0, 1), (2, 3, 1, 0))

HBM = pltpu.MemorySpace.HBM
VMEM = pltpu.MemorySpace.VMEM


def attend_kernel(q_hbm, k_hbm, v_hbm, lengths_hbm, out_ref, q_ref, k_ref, v_ref, lengths_ref, sems):
    pairs = [(lengths_hbm, lengths_ref), (q_hbm, q_ref), (k_hbm, k_ref), (v_hbm, v_ref)]
    copies = [pltpu.make_async_copy(a, b, sems.at[i]) for i, (a, b) in enumerate(pairs)]
    for copy in copies:
        copy.start()
    rows, length = k_ref.shape[:2]
    first = lax.axis_index("tp") * length
    used = GROUP * rows
    tall = -(-used // 16) * 16
    scale = 1.0 / (HEAD_DIM**0.5)
    owner = lax.rem(lax.broadcasted_iota(jnp.int32, (tall, length), 0), rows)
    place = lax.broadcasted_iota(jnp.int32, (tall, length), 1)
    lane = lax.broadcasted_iota(jnp.int32, (tall, LANES), 1)
    home = lax.broadcasted_iota(jnp.int32, (tall, LANES), 0) // rows * KV_HEADS
    tops = jnp.zeros((tall, LANES), jnp.float32)
    sums = jnp.zeros((tall, LANES), jnp.float32)
    pad = jnp.zeros((tall - used, HEAD_DIM), jnp.float32)
    for copy in copies[:3]:
        copy.wait()
    limit = jnp.zeros((tall, length), jnp.int32)
    for b in range(rows):
        limit = jnp.where(owner == b, lengths_ref[b] - first, limit)
    live = place < limit
    q = q_ref[...].astype(jnp.float32)
    weights = []
    for k in range(KV_HEADS):
        span = pl.ds(k * HEAD_DIM, HEAD_DIM)
        heads = [slice((k * GROUP + g) * HEAD_DIM, (k * GROUP + g + 1) * HEAD_DIM) for g in range(GROUP)]
        queries = jnp.concatenate([q[:, h] for h in heads] + [pad], axis=0).astype(jnp.bfloat16)
        both = lax.dot_general(
            queries,
            k_ref[:, :, span].reshape(rows * length, HEAD_DIM),
            (((1,), (1,)), ((), ())),
            preferred_element_type=jnp.float32,
        )
        scores = both[:, :length]
        for b in range(1, rows):
            scores = jnp.where(owner == b, both[:, b * length : (b + 1) * length], scores)
        scores = jnp.where(live, scores * scale, jnp.float32(DEAD))
        top = jnp.max(scores, axis=1, keepdims=True).astype(jnp.bfloat16).astype(jnp.float32)
        expo = jnp.where(live, jnp.exp(scores - top), jnp.float32(0.0))
        here = lane == home + k
        tops = jnp.where(here, top, tops)
        sums = jnp.where(here, jnp.sum(expo, axis=1, keepdims=True), sums)
        weights.append(
            jnp.concatenate(
                [jnp.where(owner == b, expo, jnp.float32(0.0)) for b in range(rows)], axis=1
            ).astype(jnp.bfloat16)
        )
    width = HEADS * HEAD_DIM
    top = functools.reduce(jnp.add, [tops[g * rows : (g + 1) * rows] for g in range(GROUP)])
    total = functools.reduce(jnp.add, [sums[g * rows : (g + 1) * rows] for g in range(GROUP)])
    high = total.astype(jnp.bfloat16)
    low = (total - high.astype(jnp.float32)).astype(jnp.bfloat16)
    for i, part in enumerate((top.astype(jnp.bfloat16), high, low)):
        out_ref[:, width + i * LANES : width + (i + 1) * LANES] = part
    copies[3].wait()
    for k in range(KV_HEADS):
        span = pl.ds(k * HEAD_DIM, HEAD_DIM)
        out = jnp.dot(
            weights[k],
            v_ref[:, :, span].reshape(rows * length, HEAD_DIM),
            preferred_element_type=jnp.float32,
        )
        for g in range(GROUP):
            head = k * GROUP + g
            out_ref[:, head * HEAD_DIM : (head + 1) * HEAD_DIM] = (
                out[g * rows : (g + 1) * rows].astype(jnp.bfloat16)
            )


def project_kernel(sources, crossed, route_hbm, weight_ref, *refs):
    messages = refs[:sources]
    *outs, attended, route_ref, sem = refs[sources:]
    rows, cols = outs[0].shape[1:]
    depth = weight_ref.shape[0]
    fetch = pltpu.make_async_copy(route_hbm, route_ref, sem)
    fetch.start()
    tops, highs, lows = (
        [m[:, depth + i * LANES : depth + (i + 1) * LANES].astype(jnp.float32) for m in messages]
        for i in range(3)
    )
    sums = [high + low for high, low in zip(highs, lows)]
    peak = functools.reduce(jnp.maximum, tops)
    factors = [jnp.exp(top - peak) for top in tops]
    total = functools.reduce(jnp.add, [f * s for f, s in zip(factors, sums)])
    shares = [f / total for f in factors]
    attended[...] = jnp.zeros_like(attended)
    acc = jnp.zeros((attended.shape[0], cols), jnp.float32)
    for first in range(0, HEADS, PER_DOT):
        for head in range(first, first + PER_DOT):
            k, g = divmod(head, GROUP)
            lane = KV_HEADS * g + k
            span = slice(head * HEAD_DIM, (head + 1) * HEAD_DIM)
            attended[:rows, span] = functools.reduce(
                jnp.add,
                [
                    m[:, span].astype(jnp.float32) * s[:, lane : lane + 1]
                    for m, s in zip(messages, shares)
                ],
            )
        span = slice(first * HEAD_DIM, (first + PER_DOT) * HEAD_DIM)
        acc += jnp.dot(
            attended[:, span].astype(jnp.bfloat16),
            weight_ref[span, :],
            preferred_element_type=jnp.float32,
        )
    fetch.wait()
    place = lax.axis_index("grp")
    mine = place + 1 - 2 * lax.rem(place, CORES) if crossed else place
    targets = [route_ref[mine * rows + b] for b in range(rows)]
    slot_row = lax.broadcasted_iota(jnp.int32, (rows, cols), 0)

    def placed(slot):
        out = jnp.zeros((rows, cols), jnp.float32)
        for b in range(rows):
            out = jnp.where(slot_row == targets[b] - slot * rows, acc[b : b + 1], out)
        return out.astype(jnp.bfloat16)

    if len(outs) == 1:
        for slot in range(outs[0].shape[0]):
            outs[0][slot] = placed(slot)
    else:
        chip, core = place // CORES, lax.rem(place, CORES)
        outs[0][0] = placed(place)
        outs[0][1] = placed(chip * CORES + 1 - core)
        for steps, out in zip(zip(*OVER_CHIPS), outs[1:]):
            goal = sum(
                jnp.where(place == i * CORES + c, steps[c][i], 0)
                for c in range(CORES)
                for i in range(len(steps[c]))
            )
            out[0] = placed(goal * CORES + 1 - core)
            out[1] = placed(goal * CORES + core)


def relay_kernel(*refs):
    refs[-1][...] = functools.reduce(jnp.add, [r[1].astype(jnp.float32) for r in refs[:-1]]).astype(
        jnp.bfloat16
    )


def collect_kernel(*refs):
    parts = [r[0].astype(jnp.float32) for r in refs[:-2]] + [refs[-2][...].astype(jnp.float32)]
    refs[-1][...] = functools.reduce(jnp.add, parts).astype(jnp.bfloat16)


def body(tp, grp, query, key_cache, value_cache, lengths, route, out_weight):
    rows, depth = query.shape
    cols = out_weight.shape[1]
    here = pl.BlockSpec(memory_space=VMEM)
    there = pl.BlockSpec(memory_space=HBM)
    inputs = [pltpu.with_memory_space_constraint(x, HBM) for x in (query, key_cache, value_cache, lengths)]
    message = pl.pallas_call(
        attend_kernel,
        out_shape=jax.ShapeDtypeStruct((rows, depth + EXTRA), jnp.bfloat16),
        in_specs=[there] * 4,
        out_specs=here,
        scratch_shapes=[
            pltpu.VMEM(query.shape, query.dtype),
            pltpu.VMEM(key_cache.shape, key_cache.dtype),
            pltpu.VMEM(value_cache.shape, value_cache.dtype),
            pltpu.SMEM(lengths.shape, lengths.dtype),
            pltpu.SemaphoreType.DMA((4,)),
        ],
        compiler_params=pltpu.CompilerParams(vmem_limit_bytes=8 << 20),
        cost_estimate=pl.CostEstimate(
            flops=20_000_000_000, transcendentals=0, bytes_accessed=40_000_000
        ),
        name="attend",
    )(*inputs)
    crossed = tp == len(OVER_TP[0]) and grp % CORES == 0
    if crossed:
        swap = [(g, g ^ 1) for g in range(grp)]
        messages = [lax.ppermute(message, "grp", swap)]
        for step in OVER_TP:
            pairs = [(g * tp + t, (g ^ 1) * tp + step[t]) for g in range(grp) for t in range(tp)]
            messages.append(lax.ppermute(message, ("grp", "tp"), pairs))
    else:
        gathered = lax.all_gather(message, "tp", axis=0)
        messages = [gathered[i] for i in range(tp)]
    chips = len(OVER_CHIPS[0][0])
    by_steps = grp == chips * CORES
    shape = jax.ShapeDtypeStruct((CORES if by_steps else grp, rows, cols), jnp.bfloat16)
    outgoing = pl.pallas_call(
        functools.partial(project_kernel, tp, crossed),
        out_shape=[shape] * (chips if by_steps else 1),
        in_specs=[there] + [here] * (tp + 1),
        out_specs=[here] * (chips if by_steps else 1),
        scratch_shapes=[
            pltpu.VMEM((16, depth), jnp.float32),
            pltpu.SMEM(route.shape, route.dtype),
            pltpu.SemaphoreType.DMA,
        ],
        compiler_params=pltpu.CompilerParams(vmem_limit_bytes=24 << 20),
        name="project",
    )(pltpu.with_memory_space_constraint(route, HBM), out_weight, *messages)
    if not by_steps:
        incoming = lax.all_to_all(outgoing[0], "grp", 0, 0)
        return jnp.sum(incoming.astype(jnp.float32), axis=0).astype(jnp.bfloat16)
    got = [outgoing[0]]
    for steps, block in zip(zip(*OVER_CHIPS), outgoing[1:]):
        pairs = [
            (i * CORES + c, steps[c][i] * CORES + 1 - c)
            for i in range(chips)
            for c in range(CORES)
        ]
        got.append(lax.ppermute(block, "grp", pairs))
    row_block = jax.ShapeDtypeStruct((rows, cols), jnp.bfloat16)
    partners = pl.pallas_call(
        relay_kernel,
        out_shape=row_block,
        in_specs=[here] * chips,
        out_specs=here,
        compiler_params=pltpu.CompilerParams(vmem_limit_bytes=1 << 20),
        name="relay",
    )(*got)
    swap = [(i, i ^ 1) for i in range(grp)]
    return pl.pallas_call(
        collect_kernel,
        out_shape=row_block,
        in_specs=[here] * (chips + 1),
        out_specs=here,
        compiler_params=pltpu.CompilerParams(vmem_limit_bytes=1 << 20),
        name="collect",
    )(*got, lax.ppermute(partners, "grp", swap))


def solution(mesh):
    return jax.shard_map(
        functools.partial(body, mesh.shape["tp"], mesh.shape["grp"]),
        mesh=mesh,
        in_specs=(
            P("grp", None),
            P("grp", "tp", None),
            P("grp", "tp", None),
            P("grp"),
            P(),
            P(None, "tp"),
        ),
        out_specs=P("grp", "tp"),
        check_vma=False,
    )
```
